8 devices in a mesh: dp: 1 (over z), tp: 8 (over x, y, core).
Axes of the slice: x: 2, y: 2, z: 1, core: 2. Of those that a mesh axis runs over, the one named last changes fastest.
Arguments:
- x: bfloat16 [1, 3072, 3584], P('dp', 'tp')
- dy: bfloat16 [1, 3072, 3584], P('dp', 'tp')
- wq: bfloat16 [3584, 4096], P(None, 'tp')
- wk: bfloat16 [3584, 2048], P(None, 'tp')
- wv: bfloat16 [3584, 2048], P(None, 'tp')
- wo: bfloat16 [4096, 3584], P('tp')
- w_gate: bfloat16 [3584, 14336], P(None, 'tp')
- w_up: bfloat16 [3584, 14336], P(None, 'tp')
- w_down: bfloat16 [14336, 3584], P('tp')
Outputs:
- output 1: bfloat16 [1, 3072, 3584], P('dp', 'tp')
- output 2: bfloat16 [3584, 4096], P('dp', 'tp')
- output 3: bfloat16 [3584, 2048], P('dp', 'tp')
- output 4: bfloat16 [3584, 2048], P('dp', 'tp')
- output 5: bfloat16 [4096, 3584], P(('dp', 'tp'))
- output 6: bfloat16 [3584, 14336], P('dp', 'tp')
- output 7: bfloat16 [3584, 14336], P('dp', 'tp')
- output 8: bfloat16 [14336, 3584], P(('dp', 'tp'))
All inputs are finite; a program needn't handle non-finite values.
Results may differ from the reference program's by a relative error of at most 0.024.
Values are sent between devices in bfloat16 or wider.
A program may use at most 2 GiB of HBM per device.

```python
import jax
import jax.numpy as jnp
from jax import lax

SEQUENCES = 1
TOKENS = 3072
D = 3584
HEADS = 16
KV_HEADS = 8
HEAD = 256
FF = 14336
THETA = 10000
NAMES = ("wq", "wk", "wv", "wo", "w_gate", "w_up", "w_down")
SHAPES = {
    "wq": (D, HEADS * HEAD),
    "wk": (D, KV_HEADS * HEAD),
    "wv": (D, KV_HEADS * HEAD),
    "wo": (HEADS * HEAD, D),
    "w_gate": (D, FF),
    "w_up": (D, FF),
    "w_down": (FF, D),
}


def bump(key, n, height):
    away = (jnp.arange(n, dtype=jnp.int32) - jax.random.randint(key, (), 0, n, jnp.int32)) % n
    return jnp.where(away < n // 8, height, 1.0)


def together(key, own, strength):
    shared = jax.random.normal(key, own.shape[1:], jnp.float32)
    return (own + strength * shared) * lax.rsqrt(1 + strength * strength)


def setup_inputs(seed: int = 0, part: int = 0) -> dict:
    kx, kdy, ka, kb, kz, kf, kh, kl, *kw = jax.random.split(jax.random.key(seed), 8 + len(NAMES))
    kx, kdy, ka, kb = (jax.random.fold_in(k, part) for k in (kx, kdy, ka, kb))
    shape = (SEQUENCES, TOKENS, D)
    much_x, much_dy = jax.random.uniform(kz, (2,), jnp.float32, 0.0, 1.0)
    loud = 2.0 ** jax.random.uniform(jax.random.fold_in(kz, 1), (), jnp.float32, -1.0, 2.0)
    halves = 2.0 ** jax.random.uniform(kl, (2,), jnp.float32, -1.0, 1.0)
    times = {"wq": 1.0, "wk": 1.0, "wv": 2.0, "wo": halves[0], "w_gate": 1.0, "w_up": bump(kh, FF, 4.0), "w_down": halves[1]}
    x = together(ka, jax.random.normal(kx, shape, jnp.float32), much_x) * bump(kf, D, 4.0)
    dy = together(kb, jax.random.normal(kdy, shape, jnp.float32), much_dy)
    drawn = {"x": x.astype(jnp.bfloat16), "dy": (loud * dy * (SEQUENCES * TOKENS) ** -0.5).astype(jnp.bfloat16)}
    for key, name in zip(kw, NAMES, strict=True):
        drawn[name] = (jax.random.normal(key, SHAPES[name], jnp.float32) * SHAPES[name][0] ** -0.5 * times[name]).astype(jnp.bfloat16)
    return drawn


def matmul(a, w):
    return jnp.dot(a, w, preferred_element_type=jnp.float32).astype(jnp.bfloat16)


def normed(h):
    wide = h.astype(jnp.float32)
    scale = lax.rsqrt(jnp.mean(wide**2, -1, keepdims=True) + 1e-6)
    return (wide * scale).astype(jnp.bfloat16)


def turned(t, theta):
    half = t.shape[-1] // 2
    angle = jnp.arange(t.shape[0], dtype=jnp.float32)[:, None] * theta ** (-jnp.arange(half, dtype=jnp.float32) / half)
    cos, sin = jnp.cos(angle)[:, None], jnp.sin(angle)[:, None]
    a, b = t[..., :half].astype(jnp.float32), t[..., half:].astype(jnp.float32)
    return jnp.concatenate([a * cos - b * sin, b * cos + a * sin], -1).astype(jnp.bfloat16)


def seen_by(q, k, v):
    tokens, kv = q.shape[0], k.shape[1]
    q = q.reshape(tokens, kv, -1, q.shape[-1])
    scores = jnp.einsum("tgsd,ugd->gstu", q.astype(jnp.float32), k.astype(jnp.float32)) * q.shape[-1] ** -0.5
    place = jnp.arange(tokens)
    weights = jax.nn.softmax(jnp.where(place[:, None] >= place, scores, -jnp.inf), -1).astype(jnp.bfloat16)
    return jnp.einsum("gstu,ugd->tgsd", weights.astype(jnp.float32), v.astype(jnp.float32)).astype(jnp.bfloat16).reshape(tokens, -1)


def layer(h, w):
    a = normed(h)
    q, k = (turned(matmul(a, w[name]).reshape(h.shape[0], -1, HEAD), THETA) for name in ("wq", "wk"))
    h = h + matmul(seen_by(q, k, matmul(a, w["wv"]).reshape(h.shape[0], -1, HEAD)), w["wo"])
    b = normed(h)
    gate = jnp.dot(b, w["w_gate"], preferred_element_type=jnp.float32)
    up = jnp.dot(b, w["w_up"], preferred_element_type=jnp.float32)
    return h + matmul((jax.nn.silu(gate) * up).astype(jnp.bfloat16), w["w_down"])


def reference(x, dy, wq, wk, wv, wo, w_gate, w_up, w_down):
    weights = dict(zip(NAMES, (wq, wk, wv, wo, w_gate, w_up, w_down), strict=True))

    def take(so_far, sequence):
        h, by_y = sequence
        _, back = jax.vjp(lambda w, h: layer(h, w), weights, h)
        by_weights, by_h = back(by_y)
        return jax.tree.map(lambda total, term: total + term.astype(jnp.float32), so_far, by_weights), by_h

    none_yet = {name: jnp.zeros(w.shape, jnp.float32) for name, w in weights.items()}
    by_weights, by_x = lax.scan(take, none_yet, (x, dy))
    return (by_x, *(by_weights[name].astype(jnp.bfloat16) for name in NAMES))
```

```python
import functools

import jax
import jax.numpy as jnp
from jax import lax
from jax.experimental import pallas as pl
from jax.experimental.pallas import tpu as pltpu
from jax.sharding import PartitionSpec as P

NEG = -1e30
HIDDEN = 2 * NEG
LOG2E = 1.4426950408889634
LIMIT = 67043328
STRIP = 512
HEAD = 256
HALF = HEAD // 2
QUERIES = 2
THETA = 10000
DEVICES = 8
BLOCK = 384
TOKENS = DEVICES * BLOCK
SCALE = HEAD**-0.5
LOW = jnp.bfloat16
WIDE = jnp.float32
NATURAL = tuple(range(DEVICES))
IN_ORDER = ((0, 1), (2, 3, 4, 5), (6, 7))
BY_ARRIVAL = ((0, 1), (2, 4), (3, 5, 6, 7))
ARRIVAL = sum(BY_ARRIVAL, ())


def dot(a, b, ca=1, cb=0):
    return lax.dot_general(a, b, (((ca,), (cb,)), ((), ())), preferred_element_type=WIDE)


def rounded(total, *arrived):
    for t in arrived:
        total = total + t.astype(WIDE)
    return total.astype(LOW)


def params():
    return pltpu.CompilerParams(dimension_semantics=("arbitrary",), vmem_limit_bytes=LIMIT)


def _masks(bq, bk):
    cols = QUERIES * bq
    return lax.rem(lax.broadcasted_iota(jnp.int32, (bk, cols), 1), bq) - lax.broadcasted_iota(jnp.int32, (bk, cols), 0)


def _blocks(iq, bq, bk, block):
    whole, last = lax.div(iq * bq + 1, bk), lax.div(iq * bq + bq + bk - 1, bk)
    lax.fori_loop(0, whole, lambda j, _: block(j, False), None)
    lax.fori_loop(whole, last, lambda j, _: block(j, True), None)


def _row(ref):
    return jnp.concatenate([ref[n : n + 1, :] for n in range(QUERIES)], axis=1)


def _forward(q_ref, k_ref, v_ref, o_ref, lse_ref, top_s, mix_s, gap_s, *, bq, bk):
    cols = QUERIES * bq
    iq = pl.program_id(0)
    e = SCALE * LOG2E
    pieces = range(0, cols, STRIP)

    @pl.when(iq == 0)
    def _():
        gap_s[...] = _masks(bq, bk)

    top_s[...] = jnp.full((1, cols), NEG, WIDE)
    mix_s[...] = jnp.zeros_like(mix_s)
    ones = jnp.ones((8, bk), LOW)

    def block(j, masked):
        here = pl.ds(j * bk, bk)
        scores = [dot(k_ref[here, :], q_ref[...].reshape(cols, HEAD)[at : at + STRIP, :], 1, 1) for at in pieces]
        ok = gap_s[...] >= j * bk - iq * bq if masked else None
        weights, keeps = [], []
        for at, s in zip(pieces, scores):
            if masked:
                s = jnp.where(ok[:, at : at + STRIP], s, HIDDEN)
            old = top_s[:, at : at + STRIP]
            top = jnp.maximum(old, s.max(axis=0, keepdims=True))
            top_s[:, at : at + STRIP] = top
            weights.append(jnp.exp2((s - top) * e).astype(LOW))
            keeps.append(jnp.exp2((old - top) * e))
        for at, p, keep in zip(pieces, weights, keeps):
            values = jnp.concatenate([v_ref[here, :].T, ones], axis=0)
            mix_s[:, at : at + STRIP] = mix_s[:, at : at + STRIP] * keep + dot(values, p)

    _blocks(iq, bq, bk, block)
    total = mix_s[HEAD : HEAD + 1, :]
    o_ref[...] = (mix_s[:HEAD, :] * (1 / total)).T.reshape(QUERIES, bq, HEAD).astype(LOW)
    lse = top_s[...] * SCALE + jnp.log(total)
    for n in range(QUERIES):
        lse_ref[n : n + 1, :] = lse[:, n * bq : (n + 1) * bq]


def _queries(bq):
    return pl.BlockSpec((QUERIES, bq, HEAD), lambda i: (0, i, 0)), pl.BlockSpec((QUERIES, bq), lambda i: (0, i))


def _whole(*shape):
    return pl.BlockSpec(shape, lambda i: (0,) * len(shape))


def _attention_cost(width):
    n = QUERIES * TOKENS * TOKENS
    return pl.CostEstimate(flops=n * width * HEAD, transcendentals=n // 2, bytes_accessed=12 * TOKENS * HEAD)


def attend(q, k, v, bq=768, bk=768):
    heads, stats = _queries(bq)
    return pl.pallas_call(
        functools.partial(_forward, bq=bq, bk=bk),
        grid=(TOKENS // bq,),
        in_specs=[heads, _whole(TOKENS, HEAD), _whole(TOKENS, HEAD)],
        out_specs=[heads, stats],
        out_shape=[jax.ShapeDtypeStruct(q.shape, LOW), jax.ShapeDtypeStruct(q.shape[:2], WIDE)],
        scratch_shapes=[pltpu.VMEM((1, QUERIES * bq), WIDE), pltpu.VMEM((HEAD + 8, QUERIES * bq), WIDE), pltpu.VMEM((bk, QUERIES * bq), jnp.int32)],
        compiler_params=params(),
        cost_estimate=_attention_cost(2),
    )(q, k, v)


def _backward(q_ref, k_ref, v_ref, do_ref, lse_ref, delta_ref, dq_ref, dk_ref, dv_ref, dq_s, dk_s, dv_s, gap_s, *, bq, bk):
    cols = QUERIES * bq
    iq = pl.program_id(0)
    e = SCALE * LOG2E
    pieces = range(0, cols, STRIP)

    @pl.when(iq == 0)
    def _():
        gap_s[...] = _masks(bq, bk)
        dk_s[...] = jnp.zeros_like(dk_s)
        dv_s[...] = jnp.zeros_like(dv_s)

    dq_s[...] = jnp.zeros_like(dq_s)
    lses = _row(lse_ref) * LOG2E
    deltas = _row(delta_ref)

    def block(j, masked):
        here = pl.ds(j * bk, bk)
        qs = [q_ref[...].reshape(cols, HEAD)[at : at + STRIP, :] for at in pieces]
        dos = [do_ref[...].reshape(cols, HEAD)[at : at + STRIP, :] for at in pieces]
        scores = [dot(k_ref[here, :], x, 1, 1) for x in qs]
        dps = [dot(v_ref[here, :], x, 1, 1) for x in dos]
        ok = gap_s[...] >= j * bk - iq * bq if masked else None
        for n, at in enumerate(pieces):
            p = jnp.exp2(scores[n] * e - lses[:, at : at + STRIP])
            if masked:
                p = jnp.where(ok[:, at : at + STRIP], p, 0.0)
            ds = (p * (dps[n] - deltas[:, at : at + STRIP])).astype(LOW)
            dv_s[here, :] += dot(p.astype(LOW), dos[n])
            dk_s[here, :] += dot(ds, qs[n])
            dq_s[:, at : at + STRIP] += dot(k_ref[here, :].T, ds)

    _blocks(iq, bq, bk, block)
    dq_ref[...] = (dq_s[...] * SCALE).T.reshape(QUERIES, bq, HEAD).astype(LOW)

    @pl.when(iq == pl.num_programs(0) - 1)
    def _():
        dk_ref[...] = (dk_s[...] * SCALE).astype(LOW)
        dv_ref[...] = dv_s[...].astype(LOW)


def attend_back(q, k, v, d_out, lse, delta, bq=512, bk=512):
    heads, stats = _queries(bq)
    keys = _whole(TOKENS, HEAD)
    return pl.pallas_call(
        functools.partial(_backward, bq=bq, bk=bk),
        grid=(TOKENS // bq,),
        in_specs=[heads, keys, keys, heads, stats, stats],
        out_specs=[heads, keys, keys],
        out_shape=[jax.ShapeDtypeStruct(t.shape, LOW) for t in (q, k, v)],
        scratch_shapes=[pltpu.VMEM((HEAD, QUERIES * bq), WIDE), pltpu.VMEM((TOKENS, HEAD), WIDE), pltpu.VMEM((TOKENS, HEAD), WIDE),
                        pltpu.VMEM((bk, QUERIES * bq), jnp.int32)],
        compiler_params=params(),
        cost_estimate=_attention_cost(5),
    )(q, k, v, d_out, lse, delta)


def _of_groups(refs, groups, store):
    first = 0
    for ref, group in zip(refs, groups):
        last = first + len(group)
        pl.when((pl.program_id(0) >= first) & (pl.program_id(0) < last))(functools.partial(store, ref))
        first = last


def _turn(own_ref, *refs):
    groups, (cos_ref, sin_ref, q_ref, k_ref, v_ref) = refs[:-5], refs[-5:]

    def store(t_ref):
        cos, sin = cos_ref[...], sin_ref[...]
        for n, to in enumerate((q_ref.at[0], q_ref.at[1], k_ref)):
            a = t_ref[:, n * HEAD : n * HEAD + HALF].astype(WIDE)
            b = t_ref[:, n * HEAD + HALF : (n + 1) * HEAD].astype(WIDE)
            to[:, :HALF] = (a * cos - b * sin).astype(LOW)
            to[:, HALF:] = (b * cos + a * sin).astype(LOW)
        v_ref[...] = t_ref[:, 3 * HEAD :]

    _of_groups(groups, IN_ORDER, store)


def _turn_back(own_ref, q_ref, k_ref, v_ref, cos_ref, sin_ref, t_ref):
    cos, sin = cos_ref[...], sin_ref[...]
    for n, of in enumerate((q_ref.at[0], q_ref.at[1], k_ref)):
        a, b = of[:, :HALF].astype(WIDE), of[:, HALF:].astype(WIDE)
        t_ref[:, n * HEAD : n * HEAD + HALF] = (a * cos + b * sin).astype(LOW)
        t_ref[:, n * HEAD + HALF : (n + 1) * HEAD] = (b * cos - a * sin).astype(LOW)
    t_ref[:, 3 * HEAD :] = v_ref[...]


def _to_places(own_ref, t_ref, o_ref):
    for n in range(QUERIES):
        o_ref[:, n * HEAD : (n + 1) * HEAD] = t_ref[n]


def _to_tokens(own_ref, *refs):
    o_ref = refs[-1]

    def store(t_ref):
        for n in range(QUERIES):
            o_ref[n] = t_ref[:, n * HEAD : (n + 1) * HEAD]

    _of_groups(refs[:-1], BY_ARRIVAL, store)


def by_blocks(kernel, given, outs, groups=(NATURAL,)):
    sizes = [len(group) for group in groups]
    spans = iter([(sum(sizes[:n]), size) for n, size in enumerate(sizes)])

    def spec(shape):
        if len(shape) == 3:
            return pl.BlockSpec((shape[0], BLOCK, shape[2]), lambda s, own: (0, own[s], 0))
        if shape[1] <= HEAD:
            return pl.BlockSpec((BLOCK, shape[1]), lambda s, own: (own[s], 0))
        first, size = next(spans)
        return pl.BlockSpec((BLOCK, shape[1]), lambda s, own: (jnp.clip(s - first, 0, size - 1), 0))

    size = sum(2 * a.size for a in given)
    return pl.pallas_call(
        kernel,
        grid_spec=pltpu.PrefetchScalarGridSpec(num_scalar_prefetch=1, grid=(DEVICES,), in_specs=[spec(a.shape) for a in given],
                                               out_specs=[spec(s) for s in outs]),
        out_shape=[jax.ShapeDtypeStruct(s, LOW) for s in outs],
        compiler_params=params(),
        cost_estimate=pl.CostEstimate(flops=4 * size, transcendentals=0, bytes_accessed=2 * size),
    )(owners(sum(groups, ())), *given)


HBM = pl.BlockSpec(memory_space=pltpu.HBM)


class Turns:
    def __init__(self):
        self.last = []

    def done(self, *results):
        self.last = list(results)


class Sources:
    def __init__(self, turns):
        self.arrays = []
        self.turns = turns

    def add(self, piece):
        t, at, n = piece
        for i, other in enumerate(self.arrays):
            if other is t:
                return i, at, n
        self.arrays.append(t)
        return len(self.arrays) - 1, at, n

    def close(self):
        for t in self.turns.last:
            self.add((t, 0, 0))


def _fetch(refs, pieces, to, sem, columns=slice(None)):
    copies, row = [], 0
    for i, (which, at, n) in enumerate(pieces):
        copies.append(pltpu.make_async_copy(refs[which].at[pl.ds(at, n), columns], to.at[pl.ds(row, n), :], sem.at[i]))
        row += n
    return copies


def _start(copies):
    for c in copies:
        c.start()


def _wait(copies):
    for c in copies:
        c.wait()


def _spans(pieces):
    row = 0
    for _, _, n in pieces:
        yield row, n
        row += n


def _tile_of(step, tile):
    return pl.ds(pl.multiple_of(step * tile, tile), tile)


def rows_times(turns, lhs, weights, flip, tile, finish, given, outs):
    sources = Sources(turns)
    lhs = [[sources.add(p) for p in pieces] for pieces in lhs]
    sources.close()
    spans = list(_spans(lhs[0]))
    total_rows = sum(n for _, n in spans)
    widths = [w.shape[1] if flip else w.shape[0] for w in weights]
    n_out = weights[0].shape[0] if flip else weights[0].shape[1]
    n_src, n_w, n_l, n_in = len(sources.arrays), len(weights), len(lhs), len(given)
    steps = n_out // tile

    def kernel(*refs):
        src, ws, ins, rest = refs[:n_src], refs[n_src : n_src + n_w], refs[n_src + n_w : n_src + n_w + n_in], refs[n_src + n_w + n_in :]
        out_refs, rest = rest[: len(outs)], rest[len(outs) :]
        held, slots, sems, slot_sem = rest[:n_l], rest[n_l : n_l + n_w], rest[n_l + n_w : -1], rest[-1]
        j = pl.program_id(0)
        slot = lax.rem(j, 2)

        def tiles(step, slot):
            here = _tile_of(step, tile)
            return [pltpu.make_async_copy(w.at[here, :] if flip else w.at[:, here], s.at[slot], slot_sem.at[slot, i])
                    for i, (w, s) in enumerate(zip(ws, slots))]

        def multiply(row, n):
            here = pl.ds(row, n)
            terms = [dot(held[min(i, n_l - 1)][here, :], slots[i][slot], 1, 1 if flip else 0) for i in range(n_w)]
            finish(terms, row, n, ins, out_refs)

        @pl.when(j == 0)
        def _():
            copies = [_fetch(src, pieces, to, sem) for pieces, to, sem in zip(lhs, held, sems)]
            first = tiles(0, 0)
            _start([first[0], *(c[0] for c in copies), *first[1:]])
            for i in range(1, len(spans)):
                _start([c[i] for c in copies])
            _wait(first)
            for i, span in enumerate(spans):
                _wait([c[i] for c in copies])
                if i == len(spans) - 1 and steps > 1:
                    _start(tiles(1, 1))
                multiply(*span)

        @pl.when((j > 0) & (j + 1 < steps))
        def _():
            _start(tiles(j + 1, 1 - slot))

        @pl.when(j > 0)
        def _():
            _wait(tiles(j, slot))
            for row in range(0, total_rows, 2 * BLOCK):
                multiply(row, 2 * BLOCK)

    columns = lambda n: pl.BlockSpec((n, tile), lambda j: (0, j))
    wide = sum(widths)
    got = pl.pallas_call(
        kernel,
        grid=(steps,),
        in_specs=[HBM] * (n_src + n_w) + [columns(t.shape[0]) for t in given],
        out_specs=[columns(n) for n in outs],
        out_shape=[jax.ShapeDtypeStruct((n, n_out), LOW) for n in outs],
        scratch_shapes=[pltpu.VMEM((total_rows, w), LOW) for w in widths[:n_l]]
        + [pltpu.VMEM((2, tile, w) if flip else (2, w, tile), LOW) for w in widths]
        + [pltpu.SemaphoreType.DMA((len(spans),))] * n_l + [pltpu.SemaphoreType.DMA((2, n_w))],
        compiler_params=params(),
        cost_estimate=pl.CostEstimate(flops=2 * total_rows * wide * n_out, transcendentals=0,
                                      bytes_accessed=2 * (wide * n_out + total_rows * (wide + n_out))),
    )(*sources.arrays, *weights, *given)
    turns.done(got[-1])
    return got


def product(turns, lhs, weights, flip, arrived=None, tile=512, joint=False):
    sizes = [n for _, _, n in lhs[0]]
    arrived = arrived or [()] * len(sizes)

    def finish(terms, row, n, ins, outs):
        total = sum(terms[1:], terms[0])
        if joint:
            outs[0][pl.ds(row, n), :] = total.astype(LOW)
            return
        ins = iter(ins)
        for (at, size), ts, out in zip(_spans(lhs[0]), arrived, outs):
            mine = [next(ins) for _ in ts]
            if row <= at < row + n:
                out[...] = rounded(total[at - row : at - row + size], *(t[...] for t in mine))

    got = rows_times(turns, lhs, weights, flip, tile, finish, [t for ts in arrived for t in ts], [sum(sizes)] if joint else sizes)
    return got[0] if joint else got


def gated(turns, pieces, w_gate, w_up, back):
    def finish(terms, row, n, ins, outs):
        gate, up = terms
        here = pl.ds(row, n)
        by = ins[0][here, :].astype(WIDE)
        s = jax.nn.sigmoid(gate)
        silu = gate * s
        outs[0][here, :] = (silu * up).astype(LOW)
        outs[1][here, :] = (by * up * (s + silu * (1 - s))).astype(LOW)
        outs[2][here, :] = (by * silu).astype(LOW)

    return rows_times(turns, [pieces], [w_gate, w_up], False, HEAD, finish, [back], [back.shape[0]] * 3)


def weight_gradient(turns, lhs, rhs, hold_lhs, tile=512, splits=None, first=0, last=None, into=None):
    sources = Sources(turns)
    lhs, rhs = [sources.add(p) for p in lhs], [sources.add(p) for p in rhs]
    sources.close()
    n_src = len(sources.arrays)
    wide_l, wide_r = (sources.arrays[t[0][0]].shape[1] for t in (lhs, rhs))
    kept, tiled = (lhs, rhs) if hold_lhs else (rhs, lhs)
    wide_kept, wide_tiled = (wide_l, wide_r) if hold_lhs else (wide_r, wide_l)
    end = wide_tiled // tile if last is None else last
    splits = splits or (wide_r,)

    def kernel(*refs):
        src = refs[:n_src]
        outs = refs[n_src + (into is not None) :][: len(splits)]
        turned, held, slots, sem, slot_sems = refs[-5:]
        i = pl.program_id(0) + first
        slot = lax.rem(i, 2)

        def tiles(step, slot):
            return _fetch(src, tiled, slots.at[slot], slot_sems.at[slot], _tile_of(step, tile))

        def store(total):
            at = 0
            for ref, n in zip(outs, splits if not hold_lhs else (tile,)):
                ref[...] = total[:, at : at + n].astype(LOW)
                at += n

        @pl.when(i == first)
        def _():
            keep, now = _fetch(src, kept, held, sem), tiles(first, first % 2)
            where = list(_spans(tiled))
            for c, (row, n) in zip(keep, _spans(kept)):
                _start([c] + [t for t, (at, _) in zip(now, where) if row <= at < row + n])
            if first + 1 < end:
                _start(tiles(first + 1, 1 - first % 2))
            total = None
            for c, (row, n) in zip(keep, _spans(kept)):
                _wait([c] + [t for t, (at, _) in zip(now, where) if row <= at < row + n])
                here = pl.ds(row, n)
                if hold_lhs:
                    turned[:, here] = held[here, :].T
                    term = dot(turned[:, here], slots[first % 2, here, :])
                else:
                    term = dot(slots[first % 2, here, :], held[here, :], 0, 0)
                total = term if total is None else total + term
            store(total)

        @pl.when((i > first) & (i + 1 < end))
        def _():
            _start(tiles(i + 1, 1 - slot))

        @pl.when(i > first)
        def _():
            _wait(tiles(i, slot))
            store(dot(turned[...], slots[slot]) if hold_lhs else dot(slots[slot], held[...], 0, 0))

    if hold_lhs:
        out_specs, out_shape = [pl.BlockSpec((wide_l, tile), lambda i: (0, i + first))], [(wide_l, wide_r)]
    else:
        out_specs, out_shape = [pl.BlockSpec((tile, n), lambda i: (i + first, 0)) for n in splits], [(wide_l, n) for n in splits]
    done = tile * (end - first)
    got = pl.pallas_call(
        kernel,
        grid=(end - first,),
        in_specs=[HBM] * (n_src + (into is not None)),
        input_output_aliases={} if into is None else {n_src: 0},
        out_specs=out_specs,
        out_shape=[jax.ShapeDtypeStruct(s, LOW) for s in out_shape],
        scratch_shapes=[pltpu.VMEM((wide_l, TOKENS) if hold_lhs else (8, HALF), LOW), pltpu.VMEM((TOKENS, wide_kept), LOW), pltpu.VMEM((2, TOKENS, tile), LOW),
                        pltpu.SemaphoreType.DMA((len(kept),)), pltpu.SemaphoreType.DMA((2, len(tiled)))],
        compiler_params=params(),
        cost_estimate=pl.CostEstimate(flops=2 * TOKENS * wide_kept * done, transcendentals=0,
                                      bytes_accessed=2 * (TOKENS * wide_kept + (TOKENS + wide_kept) * done)),
    )(*sources.arrays, *([] if into is None else [into]))
    turns.done(got[0])
    return got[0] if len(got) == 1 else got


def wholes(ts):
    return [(t, 0, t.shape[0]) for t in ts]


def places(t, ps, n=1):
    return [(t, p * BLOCK, n * BLOCK) for p in ps]


def _u(i):
    return 2 if i % 2 else 4


TO_CORE = [(i, i ^ 1) for i in range(DEVICES)]
TO_U = [(i, i ^ _u(i)) for i in range(DEVICES)]
TO_V = [(i, i ^ (6 - _u(i))) for i in range(DEVICES)]


def send(t, pairs):
    return lax.ppermute(t, "tp", pairs)


def owners(order):
    me = lax.axis_index("tp")
    v = 2 + 2 * (me % 2)
    away = (0, 1, v, v ^ 1, 6 - v, 7 - v, 6, 7)
    return jnp.stack([me ^ away[p] for p in order]).astype(jnp.int32)


def gather(t, behind=None):
    out = t if behind is None else lax.optimization_barrier((t, behind))[0]
    c, u, v = send(t, TO_CORE), send(out, TO_U), send(out, TO_V)
    far = send(v, TO_U)
    return [t, c, v, send(u, TO_CORE), u, send(v, TO_CORE), far, send(far, TO_CORE)]


def scatter(turns, term, meanwhile):
    far, to_core = term((6, 7), ((), ()))
    far_core = send(to_core, TO_CORE)
    v3, u5 = term((3, 5), ((), ()))
    far = rounded(far.astype(WIDE), far_core)
    turns.done(v3, far)
    far = send(far, TO_U)
    v3, u5 = send(v3, TO_CORE), send(u5, TO_CORE)
    via_u, to_core = term((4, 1), ((v3,), ()))
    via_u, to_core = send(via_u, TO_U), send(to_core, TO_CORE)
    meanwhile()
    via_v, mine = term((2, 0), ((u5, far), ()))
    via_v = send(via_v, TO_V)
    return lambda: rounded(mine.astype(WIDE), to_core, via_u, via_v)


def normed(h):
    wide = h.astype(WIDE)
    scale = lax.rsqrt(jnp.mean(wide**2, -1, keepdims=True) + 1e-6)
    return (wide * scale).astype(LOW)


def angles():
    angle = jnp.arange(TOKENS, dtype=WIDE)[:, None] * THETA ** (-jnp.arange(HALF, dtype=WIDE) / HALF)
    return jnp.cos(angle), jnp.sin(angle)


def layer(x, dy, wq, wk, wv, wo, w_gate, w_up, w_down):
    turns = Turns()
    tables = angles()
    w_qkv = jnp.concatenate([wq, wk, wv], 1)
    turns.done(*tables)

    def by_group(n, groups, of, weight, flip, tile=512):
        return product(turns, [wholes([of[p] for p in groups[n]])], [weight], flip, joint=True, tile=tile)

    a = gather(normed(x))
    dys = gather(dy, a[6])
    qkv = [by_group(0, IN_ORDER, a, w_qkv, False)]
    by_hidden = [by_group(0, BY_ARRIVAL, dys, w_down, True, HEAD)]
    qkv += [by_group(n, IN_ORDER, a, w_qkv, False) for n in (1, 2)]
    q, k, v = by_blocks(_turn, (*qkv, *tables), ((QUERIES, TOKENS, HEAD), (TOKENS, HEAD), (TOKENS, HEAD)), IN_ORDER)
    out, lse = attend(q, k, v)
    (heads,) = by_blocks(_to_places, (out,), ((TOKENS, QUERIES * HEAD),))
    turns.done(heads)

    def hidden_back(n):
        by_hidden.append(by_group(n, BY_ARRIVAL, dys, w_down, True, HEAD))

    total = scatter(turns, lambda ps, arrived: product(turns, [places(heads, ps)], [wo], False, arrived, tile=wo.shape[1]), lambda: hidden_back(1))
    hidden_back(2)
    h = x + total()

    normed_h, norm_back = jax.vjp(normed, h)
    b = gather(normed_h)
    hidden, by_gate, by_up = [], [], []
    for n, group in enumerate(BY_ARRIVAL):
        for ts, t in zip((hidden, by_gate, by_up), gated(turns, wholes([b[p] for p in group]), w_gate, w_up, by_hidden[n])):
            ts.append(t)

    def of_groups(ts, ps):
        return [next((t, group.index(p) * BLOCK, BLOCK) for t, group in zip(ts, BY_ARRIVAL) if p in group) for p in ps]

    def arranged(ts):
        return wholes([ts[p] for p in ARRIVAL])

    def by_b(ps, arrived):
        return product(turns, [of_groups(by_gate, ps), of_groups(by_up, ps)], [w_gate, w_up], True, arrived)

    total = scatter(turns, by_b, lambda: None)
    d_down = weight_gradient(turns, wholes(hidden), arranged(dys), True)
    dh = dy + norm_back(total())[0]
    dhs = gather(dh)
    by_heads = [by_group(0, BY_ARRIVAL, dhs, wo, True)]
    d_gate = weight_gradient(turns, arranged(b), wholes(by_gate), False)
    by_heads.append(by_group(1, BY_ARRIVAL, dhs, wo, True))
    d_up = weight_gradient(turns, arranged(b), wholes(by_up), False, last=3)
    by_heads.append(by_group(2, BY_ARRIVAL, dhs, wo, True))
    (d_out,) = by_blocks(_to_tokens, by_heads, ((QUERIES, TOKENS, HEAD),), BY_ARRIVAL)
    delta = (d_out.astype(WIDE) * out.astype(WIDE)).sum(-1)
    dq, dk, dv = attend_back(q, k, v, d_out, lse, delta)
    (by_qkv,) = by_blocks(_turn_back, (dq, dk, dv, *tables), ((TOKENS, 4 * HEAD),))
    turns.done(by_qkv)
    pairs = range(0, DEVICES, 2)
    d_qkv = []

    def qkv_gradient():
        d_qkv.extend(weight_gradient(turns, wholes(a), places(by_qkv, pairs, 2), False, splits=(2 * HEAD, HEAD, HEAD)))

    total = scatter(turns, lambda ps, arrived: product(turns, [places(by_qkv, ps)], [w_qkv], True, arrived, tile=1792), qkv_gradient)
    d_o = weight_gradient(turns, places(heads, pairs, 2), wholes(dhs), True)
    d_up = weight_gradient(turns, arranged(b), wholes(by_up), False, first=3, into=d_up)
    dx = dh + jax.vjp(normed, x)[1](total())[0]
    return dx, *d_qkv, d_o, d_gate, d_up, d_down


def solution(mesh):
    def step(x, dy, *weights):
        dx, *by_weights = layer(x[0], dy[0], *weights)
        return dx[None], *by_weights

    states, by_columns, by_rows = P("dp", "tp", None), P(None, "tp"), P("tp", None)
    weights = (by_columns, by_columns, by_columns, by_rows, by_columns, by_columns, by_rows)
    own = tuple(P("dp", "tp") if spec == by_columns else P(("dp", "tp"), None) for spec in weights)
    return jax.shard_map(step, mesh=mesh, in_specs=(states, states, *weights), out_specs=(states, *own), check_vma=False)
```

```python
import functools

import jax
import jax.numpy as jnp
from jax import lax
from jax.experimental import pallas as pl
from jax.experimental.pallas import tpu as pltpu
from jax.sharding import PartitionSpec as P

NEG = -1e30
HIDDEN = 2 * NEG
LOG2E = 1.4426950408889634
LIMIT = 67043328
STRIP = 512
HEAD = 256
HALF = HEAD // 2
QUERIES = 2
THETA = 10000
DEVICES = 8
BLOCK = 384
TOKENS = DEVICES * BLOCK
SCALE = HEAD**-0.5
LOW = jnp.bfloat16
WIDE = jnp.float32
NATURAL = tuple(range(DEVICES))
IN_ORDER = ((0, 1), (2, 3, 4, 5), (6, 7))
BY_ARRIVAL = ((0, 1), (2, 4), (3, 5, 6, 7))
ARRIVAL = sum(BY_ARRIVAL, ())


def dot(a, b, ca=1, cb=0):
    return lax.dot_general(a, b, (((ca,), (cb,)), ((), ())), preferred_element_type=WIDE)


def rounded(total, *arrived):
    for t in arrived:
        total = total + t.astype(WIDE)
    return total.astype(LOW)


def params():
    return pltpu.CompilerParams(dimension_semantics=("arbitrary",), vmem_limit_bytes=LIMIT)


def _start(copies):
    for c in copies:
        c.start()


def _wait(copies):
    for c in copies:
        c.wait()


HBM = pl.BlockSpec(memory_space=pltpu.HBM)


def _masks(bq, bk):
    cols = QUERIES * bq
    return lax.rem(lax.broadcasted_iota(jnp.int32, (bk, cols), 1), bq) - lax.broadcasted_iota(jnp.int32, (bk, cols), 0)


def _blocks(iq, bq, bk, block):
    whole, last = lax.div(iq * bq + 1, bk), lax.div(iq * bq + bq + bk - 1, bk)
    lax.fori_loop(0, whole, lambda j, _: block(j, False), None)
    lax.fori_loop(whole, last, lambda j, _: block(j, True), None)


def _row(ref):
    return jnp.concatenate([ref[n : n + 1, :] for n in range(QUERIES)], axis=1)


def _forward(place_ref, q_ref, k_ref, v_ref, o_ref, lse_ref, top_s, mix_s, gap_s, o_s, sem, *, bq, bk):
    cols = QUERIES * bq
    iq = pl.program_id(0)
    slot, last = lax.rem(iq, 2), pl.num_programs(0) - 1
    e = SCALE * LOG2E
    pieces = range(0, cols, STRIP)

    @pl.when(iq == 0)
    def _():
        gap_s[...] = _masks(bq, bk)

    def copies(i, slot):
        per = bq // BLOCK
        return [pltpu.make_async_copy(o_s.at[slot, pl.ds(n * BLOCK, BLOCK), :], o_ref.at[pl.ds(place_ref[i * per + n] * BLOCK, BLOCK), :], sem.at[slot, n])
                for n in range(per)]

    top_s[...] = jnp.full((1, cols), NEG, WIDE)
    mix_s[...] = jnp.zeros_like(mix_s)
    ones = jnp.ones((8, bk), LOW)

    def block(j, masked):
        here = pl.ds(j * bk, bk)
        scores = [dot(k_ref[here, :], q_ref[...].reshape(cols, HEAD)[at : at + STRIP, :], 1, 1) for at in pieces]
        ok = gap_s[...] >= j * bk - iq * bq if masked else None
        weights, keeps = [], []
        for at, s in zip(pieces, scores):
            if masked:
                s = jnp.where(ok[:, at : at + STRIP], s, HIDDEN)
            old = top_s[:, at : at + STRIP]
            top = jnp.maximum(old, s.max(axis=0, keepdims=True))
            top_s[:, at : at + STRIP] = top
            weights.append(jnp.exp2((s - top) * e).astype(LOW))
            keeps.append(jnp.exp2((old - top) * e))
        for at, p, keep in zip(pieces, weights, keeps):
            values = jnp.concatenate([v_ref[here, :].T, ones], axis=0)
            mix_s[:, at : at + STRIP] = mix_s[:, at : at + STRIP] * keep + dot(values, p)

    _blocks(iq, bq, bk, block)
    total = mix_s[HEAD : HEAD + 1, :]
    mixed = (mix_s[:HEAD, :] * (1 / total)).T.astype(LOW)

    @pl.when(iq > 1)
    def _():
        _wait(copies(iq - 2, slot))

    for n in range(QUERIES):
        o_s[slot, :, n * HEAD : (n + 1) * HEAD] = mixed[n * bq : (n + 1) * bq]
    _start(copies(iq, slot))
    lse = top_s[...] * SCALE + jnp.log(total)
    for n in range(QUERIES):
        lse_ref[n : n + 1, :] = lse[:, n * bq : (n + 1) * bq]

    @pl.when(iq == last)
    def _():
        _wait(copies(iq - 1, 1 - slot) + copies(iq, slot))


def _queries(bq):
    return pl.BlockSpec((QUERIES, bq, HEAD), lambda i, *_: (0, i, 0)), pl.BlockSpec((QUERIES, bq), lambda i, *_: (0, i))


def _whole(*shape):
    return pl.BlockSpec(shape, lambda i, *_: (0,) * len(shape))


def _attention_cost(width):
    n = QUERIES * TOKENS * TOKENS
    return pl.CostEstimate(flops=n * width * HEAD, transcendentals=n // 2, bytes_accessed=12 * TOKENS * HEAD)


def attend(place, q, k, v, bq=768, bk=768):
    heads, stats = _queries(bq)
    return pl.pallas_call(
        functools.partial(_forward, bq=bq, bk=bk),
        grid_spec=pltpu.PrefetchScalarGridSpec(
            num_scalar_prefetch=1,
            grid=(TOKENS // bq,),
            in_specs=[heads, _whole(TOKENS, HEAD), _whole(TOKENS, HEAD)],
            out_specs=[HBM, stats],
            scratch_shapes=[pltpu.VMEM((1, QUERIES * bq), WIDE), pltpu.VMEM((HEAD + 8, QUERIES * bq), WIDE),
                            pltpu.VMEM((bk, QUERIES * bq), jnp.int32), pltpu.VMEM((2, bq, QUERIES * HEAD), LOW),
                            pltpu.SemaphoreType.DMA((2, bq // BLOCK))],
        ),
        out_shape=[jax.ShapeDtypeStruct((TOKENS, QUERIES * HEAD), LOW), jax.ShapeDtypeStruct(q.shape[:2], WIDE)],
        compiler_params=params(),
        cost_estimate=_attention_cost(2),
    )(place, q, k, v)


def _backward(place_ref, do_place_ref, q_ref, k_ref, v_ref, *refs, bq, bk):
    per = bq // BLOCK
    o_refs, do_refs = refs[:per], refs[per : 2 * per]
    lse_ref, dq_ref, dk_ref, dv_ref, dq_s, dk_s, dv_s, gap_s, do_s, delta_s = refs[2 * per :]
    cols = QUERIES * bq
    iq = pl.program_id(0)
    e = SCALE * LOG2E
    pieces = range(0, cols, STRIP)

    @pl.when(iq == 0)
    def _():
        gap_s[...] = _masks(bq, bk)
        dk_s[...] = jnp.zeros_like(dk_s)
        dv_s[...] = jnp.zeros_like(dv_s)

    dq_s[...] = jnp.zeros_like(dq_s)
    lses = _row(lse_ref) * LOG2E
    for n in range(QUERIES):
        for i in range(per):
            at, columns = n * bq + i * BLOCK, slice(n * HEAD, (n + 1) * HEAD)
            d_out = do_refs[i][:, columns]
            do_s[at : at + BLOCK, :] = d_out
            delta_s[:, at : at + BLOCK] = (d_out.astype(WIDE) * o_refs[i][:, columns].astype(WIDE)).T.sum(axis=0, keepdims=True)
    deltas = delta_s[...]

    def block(j, masked):
        here = pl.ds(j * bk, bk)
        qs = [q_ref[...].reshape(cols, HEAD)[at : at + STRIP, :] for at in pieces]
        dos = [do_s[at : at + STRIP, :] for at in pieces]
        scores = [dot(k_ref[here, :], x, 1, 1) for x in qs]
        dps = [dot(v_ref[here, :], x, 1, 1) for x in dos]
        ok = gap_s[...] >= j * bk - iq * bq if masked else None
        for n, at in enumerate(pieces):
            p = jnp.exp2(scores[n] * e - lses[:, at : at + STRIP])
            if masked:
                p = jnp.where(ok[:, at : at + STRIP], p, 0.0)
            ds = (p * (dps[n] - deltas[:, at : at + STRIP])).astype(LOW)
            dv_s[here, :] += dot(p.astype(LOW), dos[n])
            dk_s[here, :] += dot(ds, qs[n])
            dq_s[:, at : at + STRIP] += dot(k_ref[here, :].T, ds)

    _blocks(iq, bq, bk, block)
    dq_ref[...] = (dq_s[...] * SCALE).T.reshape(QUERIES, bq, HEAD).astype(LOW)

    @pl.when(iq == pl.num_programs(0) - 1)
    def _():
        dk_ref[...] = (dk_s[...] * SCALE).astype(LOW)
        dv_ref[...] = dv_s[...].astype(LOW)


def attend_back(place, do_place, q, k, v, out, d_out, lse, bq=768, bk=768):
    heads, stats = _queries(bq)
    keys = _whole(TOKENS, HEAD)
    per = bq // BLOCK
    outs = [pl.BlockSpec((BLOCK, QUERIES * HEAD), lambda i, place, _, n=n: (place[i * per + n], 0)) for n in range(per)]
    d_outs = [pl.BlockSpec((BLOCK, QUERIES * HEAD), lambda i, _, place, n=n: (place[i * per + n], 0)) for n in range(per)]
    return pl.pallas_call(
        functools.partial(_backward, bq=bq, bk=bk),
        grid_spec=pltpu.PrefetchScalarGridSpec(
            num_scalar_prefetch=2,
            grid=(TOKENS // bq,),
            in_specs=[heads, keys, keys, *outs, *d_outs, stats],
            out_specs=[heads, keys, keys],
            scratch_shapes=[pltpu.VMEM((HEAD, QUERIES * bq), WIDE), pltpu.VMEM((TOKENS, HEAD), WIDE), pltpu.VMEM((TOKENS, HEAD), WIDE),
                            pltpu.VMEM((bk, QUERIES * bq), jnp.int32), pltpu.VMEM((QUERIES * bq, HEAD), LOW), pltpu.VMEM((1, QUERIES * bq), WIDE)],
        ),
        out_shape=[jax.ShapeDtypeStruct(t.shape, LOW) for t in (q, k, v)],
        compiler_params=params(),
        cost_estimate=_attention_cost(5),
    )(place, do_place, q, k, v, *[out] * per, *[d_out] * per, lse)


def _of_groups(refs, groups, store):
    first = 0
    for ref, group in zip(refs, groups):
        last = first + len(group)
        pl.when((pl.program_id(0) >= first) & (pl.program_id(0) < last))(functools.partial(store, ref))
        first = last


def _turn(own_ref, *refs):
    groups, (cos_ref, sin_ref, q_ref, k_ref, v_ref) = refs[:-5], refs[-5:]

    def store(t_ref):
        cos, sin = cos_ref[...], sin_ref[...]
        for n, to in enumerate((q_ref.at[0], q_ref.at[1], k_ref)):
            a = t_ref[:, n * HEAD : n * HEAD + HALF].astype(WIDE)
            b = t_ref[:, n * HEAD + HALF : (n + 1) * HEAD].astype(WIDE)
            to[:, :HALF] = (a * cos - b * sin).astype(LOW)
            to[:, HALF:] = (b * cos + a * sin).astype(LOW)
        v_ref[...] = t_ref[:, 3 * HEAD :]

    _of_groups(groups, IN_ORDER, store)


def _turn_back(own_ref, q_ref, k_ref, v_ref, cos_ref, sin_ref, t_ref):
    cos, sin = cos_ref[...], sin_ref[...]
    for n, of in enumerate((q_ref.at[0], q_ref.at[1], k_ref)):
        a, b = of[:, :HALF].astype(WIDE), of[:, HALF:].astype(WIDE)
        t_ref[:, n * HEAD : n * HEAD + HALF] = (a * cos + b * sin).astype(LOW)
        t_ref[:, n * HEAD + HALF : (n + 1) * HEAD] = (b * cos - a * sin).astype(LOW)
    t_ref[:, 3 * HEAD :] = v_ref[...]


def by_blocks(kernel, given, outs, groups=(NATURAL,)):
    sizes = [len(group) for group in groups]
    spans = iter([(sum(sizes[:n]), size) for n, size in enumerate(sizes)])

    def spec(shape):
        if len(shape) == 3:
            return pl.BlockSpec((shape[0], BLOCK, shape[2]), lambda s, own: (0, own[s], 0))
        if shape[1] <= HEAD:
            return pl.BlockSpec((BLOCK, shape[1]), lambda s, own: (own[s], 0))
        first, size = next(spans)
        return pl.BlockSpec((BLOCK, shape[1]), lambda s, own: (jnp.clip(s - first, 0, size - 1), 0))

    size = sum(2 * a.size for a in given)
    return pl.pallas_call(
        kernel,
        grid_spec=pltpu.PrefetchScalarGridSpec(num_scalar_prefetch=1, grid=(DEVICES,), in_specs=[spec(a.shape) for a in given],
                                               out_specs=[spec(s) for s in outs]),
        out_shape=[jax.ShapeDtypeStruct(s, LOW) for s in outs],
        compiler_params=params(),
        cost_estimate=pl.CostEstimate(flops=4 * size, transcendentals=0, bytes_accessed=2 * size),
    )(owners(sum(groups, ())), *given)


class Turns:
    def __init__(self):
        self.last = []

    def done(self, *results):
        self.last = list(results)


class Sources:
    def __init__(self, turns):
        self.arrays = []
        self.turns = turns

    def add(self, piece):
        t, at, n = piece
        for i, other in enumerate(self.arrays):
            if other is t:
                return i, at, n
        self.arrays.append(t)
        return len(self.arrays) - 1, at, n

    def close(self):
        for t in self.turns.last:
            self.add((t, 0, 0))


def _fetch(refs, pieces, to, sem, columns=slice(None)):
    copies, row = [], 0
    for i, (which, at, n) in enumerate(pieces):
        copies.append(pltpu.make_async_copy(refs[which].at[pl.ds(at, n), columns], to.at[pl.ds(row, n), :], sem.at[i]))
        row += n
    return copies


def _spans(pieces):
    row = 0
    for _, _, n in pieces:
        yield row, n
        row += n


def _tile_of(step, tile):
    return pl.ds(pl.multiple_of(step * tile, tile), tile)


def rows_times(turns, lhs, weights, flip, tile, finish, given, outs, into=None, at=None):
    sources = Sources(turns)
    lhs = [[sources.add(p) for p in pieces] for pieces in lhs]
    sources.close()
    spans = list(_spans(lhs[0]))
    total_rows = sum(n for _, n in spans)
    widths = [w.shape[1] if flip else w.shape[0] for w in weights]
    n_out = weights[0].shape[0] if flip else weights[0].shape[1]
    n_src, n_w, n_l, n_in = len(sources.arrays), len(weights), len(lhs), len(given)
    steps = n_out // tile
    given_too = [] if into is None else [into]

    def kernel(*refs):
        src, ws, ins, rest = refs[:n_src], refs[n_src : n_src + n_w], refs[n_src + n_w : n_src + n_w + n_in], refs[n_src + n_w + n_in + len(given_too) :]
        out_refs, rest = rest[: len(outs)], rest[len(outs) :]
        held, slots, sems, slot_sem = rest[:n_l], rest[n_l : n_l + n_w], rest[n_l + n_w : -1], rest[-1]
        j = pl.program_id(0)
        slot = lax.rem(j, 2)

        def tiles(step, slot):
            here = _tile_of(step, tile)
            return [pltpu.make_async_copy(w.at[here, :] if flip else w.at[:, here], s.at[slot], slot_sem.at[slot, i])
                    for i, (w, s) in enumerate(zip(ws, slots))]

        def multiply(row, n):
            here = pl.ds(row, n)
            terms = [dot(held[min(i, n_l - 1)][here, :], slots[i][slot], 1, 1 if flip else 0) for i in range(n_w)]
            finish(terms, row, n, ins, out_refs)

        @pl.when(j == 0)
        def _():
            copies = [_fetch(src, pieces, to, sem) for pieces, to, sem in zip(lhs, held, sems)]
            first = tiles(0, 0)
            _start([first[0], *(c[0] for c in copies), *first[1:]])
            for i in range(1, len(spans)):
                _start([c[i] for c in copies])
            _wait(first)
            for i, span in enumerate(spans):
                _wait([c[i] for c in copies])
                if i == len(spans) - 1 and steps > 1:
                    _start(tiles(1, 1))
                multiply(*span)

        @pl.when((j > 0) & (j + 1 < steps))
        def _():
            _start(tiles(j + 1, 1 - slot))

        @pl.when(j > 0)
        def _():
            _wait(tiles(j, slot))
            for row in range(0, total_rows, 2 * BLOCK):
                multiply(row, 2 * BLOCK)

    columns = lambda n: pl.BlockSpec((n, tile), lambda j: (0, j))
    wide = sum(widths)
    got = pl.pallas_call(
        kernel,
        grid=(steps,),
        in_specs=[HBM] * (n_src + n_w) + [columns(t.shape[0]) for t in given] + [HBM] * len(given_too),
        input_output_aliases={n_src + n_w + n_in: 0} if given_too else {},
        out_specs=[columns(n) if at is None else pl.BlockSpec((n, tile), lambda j: (at, j)) for n in outs],
        out_shape=[jax.ShapeDtypeStruct((n if at is None else TOKENS, n_out), LOW) for n in outs],
        scratch_shapes=[pltpu.VMEM((total_rows, w), LOW) for w in widths[:n_l]]
        + [pltpu.VMEM((2, tile, w) if flip else (2, w, tile), LOW) for w in widths]
        + [pltpu.SemaphoreType.DMA((len(spans),))] * n_l + [pltpu.SemaphoreType.DMA((2, n_w))],
        compiler_params=params(),
        cost_estimate=pl.CostEstimate(flops=2 * total_rows * wide * n_out, transcendentals=0,
                                      bytes_accessed=2 * (wide * n_out + total_rows * (wide + n_out))),
    )(*sources.arrays, *weights, *given, *given_too)
    turns.done(got[-1])
    return got


def product(turns, lhs, weights, flip, arrived=None, tile=512, joint=False, into=None, at=None):
    sizes = [n for _, _, n in lhs[0]]
    arrived = arrived or [()] * len(sizes)

    def finish(terms, row, n, ins, outs):
        total = sum(terms[1:], terms[0])
        if joint:
            outs[0][pl.ds(row, n), :] = total.astype(LOW)
            return
        ins = iter(ins)
        for (at, size), ts, out in zip(_spans(lhs[0]), arrived, outs):
            mine = [next(ins) for _ in ts]
            if row <= at < row + n:
                out[...] = rounded(total[at - row : at - row + size], *(t[...] for t in mine))

    got = rows_times(turns, lhs, weights, flip, tile, finish, [t for ts in arrived for t in ts], [sum(sizes)] if joint else sizes, into, at)
    return got[0] if joint else got


def gated(turns, pieces, w_gate, w_up, back):
    def finish(terms, row, n, ins, outs):
        gate, up = terms
        here = pl.ds(row, n)
        by = ins[0][here, :].astype(WIDE)
        s = jax.nn.sigmoid(gate)
        silu = gate * s
        outs[0][here, :] = (silu * up).astype(LOW)
        outs[1][here, :] = (by * up * (s + silu * (1 - s))).astype(LOW)
        outs[2][here, :] = (by * silu).astype(LOW)

    return rows_times(turns, [pieces], [w_gate, w_up], False, HEAD, finish, [back], [back.shape[0]] * 3)


def weight_gradient(turns, lhs, rhs, hold_lhs, tile=512, splits=None, first=0, last=None, into=None):
    sources = Sources(turns)
    lhs, rhs = [sources.add(p) for p in lhs], [sources.add(p) for p in rhs]
    sources.close()
    n_src = len(sources.arrays)
    wide_l, wide_r = (sources.arrays[t[0][0]].shape[1] for t in (lhs, rhs))
    kept, tiled = (lhs, rhs) if hold_lhs else (rhs, lhs)
    wide_kept, wide_tiled = (wide_l, wide_r) if hold_lhs else (wide_r, wide_l)
    end = wide_tiled // tile if last is None else last
    splits = splits or (wide_r,)

    def kernel(*refs):
        src = refs[:n_src]
        outs = refs[n_src + (into is not None) :][: len(splits)]
        turned, held, slots, sem, slot_sems = refs[-5:]
        i = pl.program_id(0) + first
        slot = lax.rem(i, 2)

        def tiles(step, slot):
            return _fetch(src, tiled, slots.at[slot], slot_sems.at[slot], _tile_of(step, tile))

        def store(total):
            at = 0
            for ref, n in zip(outs, splits if not hold_lhs else (tile,)):
                ref[...] = total[:, at : at + n].astype(LOW)
                at += n

        @pl.when(i == first)
        def _():
            keep, now = _fetch(src, kept, held, sem), tiles(first, first % 2)
            where = list(_spans(tiled))
            for c, (row, n) in zip(keep, _spans(kept)):
                _start([c] + [t for t, (at, _) in zip(now, where) if row <= at < row + n])
            if first + 1 < end:
                _start(tiles(first + 1, 1 - first % 2))
            total = None
            for c, (row, n) in zip(keep, _spans(kept)):
                _wait([c] + [t for t, (at, _) in zip(now, where) if row <= at < row + n])
                here = pl.ds(row, n)
                if hold_lhs:
                    turned[:, here] = held[here, :].T
                    term = dot(turned[:, here], slots[first % 2, here, :])
                else:
                    term = dot(slots[first % 2, here, :], held[here, :], 0, 0)
                total = term if total is None else total + term
            store(total)

        @pl.when((i > first) & (i + 1 < end))
        def _():
            _start(tiles(i + 1, 1 - slot))

        @pl.when(i > first)
        def _():
            _wait(tiles(i, slot))
            store(dot(turned[...], slots[slot]) if hold_lhs else dot(slots[slot], held[...], 0, 0))

    if hold_lhs:
        out_specs, out_shape = [pl.BlockSpec((wide_l, tile), lambda i: (0, i + first))], [(wide_l, wide_r)]
    else:
        out_specs, out_shape = [pl.BlockSpec((tile, n), lambda i: (i + first, 0)) for n in splits], [(wide_l, n) for n in splits]
    done = tile * (end - first)
    got = pl.pallas_call(
        kernel,
        grid=(end - first,),
        in_specs=[HBM] * (n_src + (into is not None)),
        input_output_aliases={} if into is None else {n_src: 0},
        out_specs=out_specs,
        out_shape=[jax.ShapeDtypeStruct(s, LOW) for s in out_shape],
        scratch_shapes=[pltpu.VMEM((wide_l, TOKENS) if hold_lhs else (8, HALF), LOW), pltpu.VMEM((TOKENS, wide_kept), LOW), pltpu.VMEM((2, TOKENS, tile), LOW),
                        pltpu.SemaphoreType.DMA((len(kept),)), pltpu.SemaphoreType.DMA((2, len(tiled)))],
        compiler_params=params(),
        cost_estimate=pl.CostEstimate(flops=2 * TOKENS * wide_kept * done, transcendentals=0,
                                      bytes_accessed=2 * (TOKENS * wide_kept + (TOKENS + wide_kept) * done)),
    )(*sources.arrays, *([] if into is None else [into]))
    turns.done(got[0])
    return got[0] if len(got) == 1 else got


def wholes(ts):
    return [(t, 0, t.shape[0]) for t in ts]


def places(t, ps, n=1):
    return [(t, p * BLOCK, n * BLOCK) for p in ps]


def _u(i):
    return 2 if i % 2 else 4


TO_CORE = [(i, i ^ 1) for i in range(DEVICES)]
TO_U = [(i, i ^ _u(i)) for i in range(DEVICES)]
TO_V = [(i, i ^ (6 - _u(i))) for i in range(DEVICES)]


def send(t, pairs):
    return lax.ppermute(t, "tp", pairs)


def places_of_blocks():
    me = lax.axis_index("tp")
    away = me ^ jnp.arange(DEVICES, dtype=jnp.int32)
    crossed = (away & 1) | ((away & 2) * 2) | ((away & 4) // 2)
    place = jnp.where(me % 2 == 1, crossed, away).astype(jnp.int32)
    return place, jnp.where((place == 3) | (place == 4), 7 - place, place)


def owners(order):
    me = lax.axis_index("tp")
    v = 2 + 2 * (me % 2)
    away = (0, 1, v, v ^ 1, 6 - v, 7 - v, 6, 7)
    return jnp.stack([me ^ away[p] for p in order]).astype(jnp.int32)


def gather(t, behind=None):
    out = t if behind is None else lax.optimization_barrier((t, behind))[0]
    c, u, v = send(t, TO_CORE), send(out, TO_U), send(out, TO_V)
    far = send(v, TO_U)
    return [t, c, v, send(u, TO_CORE), u, send(v, TO_CORE), far, send(far, TO_CORE)]


def scatter(turns, term, meanwhile=None, early=None):
    far, to_core = term((6, 7), ((), ()))
    far_core = send(to_core, TO_CORE)
    v3, u5 = term((3, 5), ((), ()))
    far = rounded(far.astype(WIDE), far_core)
    turns.done(v3, far)
    far = send(far, TO_U)
    v3, u5 = send(v3, TO_CORE), send(u5, TO_CORE)
    if early is not None:
        to_core, mine = early
        via_u, via_v = term((4, 2), ((v3,), (u5,)))
        via_v = rounded(via_v.astype(WIDE), far)
        turns.done(via_v)
        return mine, send(to_core, TO_CORE), send(via_u, TO_U), send(via_v, TO_V)
    via_u, to_core = term((4, 1), ((v3,), ()))
    via_u, to_core = send(via_u, TO_U), send(to_core, TO_CORE)
    meanwhile()
    via_v, mine = term((2, 0), ((u5, far), ()))
    via_v = send(via_v, TO_V)
    return mine, to_core, via_u, via_v


def by_rows(kernel, given, n_outs, rows=64):
    spec = pl.BlockSpec((rows, given[0].shape[1]), lambda i: (i, 0))
    size = given[0].size * (len(given) + n_outs)
    return pl.pallas_call(
        kernel,
        grid=(given[0].shape[0] // rows,),
        in_specs=[spec] * len(given),
        out_specs=[spec] * n_outs,
        out_shape=[jax.ShapeDtypeStruct(given[0].shape, LOW)] * n_outs,
        compiler_params=params(),
        cost_estimate=pl.CostEstimate(flops=4 * size, transcendentals=0, bytes_accessed=2 * size),
    )(*given)


def scale_of(wide):
    return lax.rsqrt(jnp.mean(wide**2, -1, keepdims=True) + 1e-6)


def normed(h):
    wide = h.astype(WIDE)
    return (wide * scale_of(wide)).astype(LOW)


def _add_and_norm(x_ref, *refs):
    *terms, h_ref, b_ref = refs
    h = rounded(x_ref[...].astype(WIDE), rounded(*(t[...].astype(WIDE) for t in terms)))
    h_ref[...] = h
    b_ref[...] = normed(h)


def _norm_back(h_ref, before_ref, *refs):
    *terms, out_ref = refs
    by = rounded(*(t[...].astype(WIDE) for t in terms)).astype(WIDE)
    wide = h_ref[...].astype(WIDE)
    scale = scale_of(wide)
    shared = scale * scale * jnp.mean(by * wide, -1, keepdims=True)
    out_ref[...] = rounded(before_ref[...].astype(WIDE), ((by - wide * shared) * scale).astype(LOW))


def angles():
    angle = jnp.arange(TOKENS, dtype=WIDE)[:, None] * THETA ** (-jnp.arange(HALF, dtype=WIDE) / HALF)
    return jnp.cos(angle), jnp.sin(angle)


def layer(x, dy, wq, wk, wv, wo, w_gate, w_up, w_down):
    turns = Turns()
    tables = angles()
    w_qkv = jnp.concatenate([wq, wk, wv], 1)
    turns.done(*tables)
    place, arrival = places_of_blocks()

    def by_group(n, groups, of, weight, flip, tile=512, into=None, at=None):
        return product(turns, [wholes([of[p] for p in groups[n]])], [weight], flip, joint=True, tile=tile, into=into, at=at)

    a = gather(normed(x))
    dys = gather(dy, a[6])
    qkv = [by_group(0, IN_ORDER, a, w_qkv, False)]
    by_hidden = [by_group(0, BY_ARRIVAL, dys, w_down, True, HEAD)]
    qkv += [by_group(n, IN_ORDER, a, w_qkv, False) for n in (1, 2)]
    q, k, v = by_blocks(_turn, (*qkv, *tables), ((QUERIES, TOKENS, HEAD), (TOKENS, HEAD), (TOKENS, HEAD)), IN_ORDER)
    heads, lse = attend(place, q, k, v)
    turns.done(heads)

    def hidden_back(n):
        by_hidden.append(by_group(n, BY_ARRIVAL, dys, w_down, True, HEAD))

    terms = scatter(turns, lambda ps, arrived: product(turns, [places(heads, ps)], [wo], False, arrived, tile=wo.shape[1]), lambda: hidden_back(1))
    hidden_back(2)
    h, b = by_rows(_add_and_norm, (x, *terms), 2)
    b = gather(b)
    hidden, by_gate, by_up = [], [], []

    def of_groups(ts, ps):
        return [next((t, group.index(p) * BLOCK, BLOCK) for t, group in zip(ts, BY_ARRIVAL) if p in group) for p in ps]

    def arranged(ts):
        return wholes([ts[p] for p in ARRIVAL])

    def by_b(ps, arrived):
        return product(turns, [of_groups(by_gate, ps), of_groups(by_up, ps)], [w_gate, w_up], True, arrived)

    for n, group in enumerate(BY_ARRIVAL):
        for ts, t in zip((hidden, by_gate, by_up), gated(turns, wholes([b[p] for p in group]), w_gate, w_up, by_hidden[n])):
            ts.append(t)
        if n == 0:
            early = by_b((1, 0), ((), ()))

    terms = scatter(turns, by_b, early=early)
    d_down = weight_gradient(turns, wholes(hidden), arranged(dys), True)
    (dh,) = by_rows(_norm_back, (h, dy, *terms), 1)
    dhs = gather(dh)
    by_heads = by_group(0, BY_ARRIVAL, dhs, wo, True, at=0)
    d_gate = weight_gradient(turns, arranged(b), wholes(by_gate), False)
    by_heads = by_group(1, BY_ARRIVAL, dhs, wo, True, into=by_heads, at=1)
    d_up = weight_gradient(turns, arranged(b), wholes(by_up), False, last=3)
    by_heads = by_group(2, BY_ARRIVAL, dhs, wo, True, into=by_heads, at=1)
    dq, dk, dv = attend_back(place, arrival, q, k, v, heads, by_heads, lse)
    (by_qkv,) = by_blocks(_turn_back, (dq, dk, dv, *tables), ((TOKENS, 4 * HEAD),))
    turns.done(by_qkv)
    pairs = range(0, DEVICES, 2)
    d_qkv = []

    def qkv_gradient():
        d_qkv.extend(weight_gradient(turns, wholes(a), places(by_qkv, pairs, 2), False, splits=(2 * HEAD, HEAD, HEAD)))

    terms = scatter(turns, lambda ps, arrived: product(turns, [places(by_qkv, ps)], [w_qkv], True, arrived, tile=1792), qkv_gradient)
    d_o = weight_gradient(turns, places(heads, pairs, 2), wholes(dhs), True)
    d_up = weight_gradient(turns, arranged(b), wholes(by_up), False, first=3, into=d_up)
    (dx,) = by_rows(_norm_back, (x, dh, *terms), 1)
    return dx, *d_qkv, d_o, d_gate, d_up, d_down


def solution(mesh):
    def step(x, dy, *weights):
        dx, *by_weights = layer(x[0], dy[0], *weights)
        return dx[None], *by_weights

    states, by_columns, by_rows = P("dp", "tp", None), P(None, "tp"), P("tp", None)
    weights = (by_columns, by_columns, by_columns, by_rows, by_columns, by_columns, by_rows)
    own = tuple(P("dp", "tp") if spec == by_columns else P(("dp", "tp"), None) for spec in weights)
    return jax.shard_map(step, mesh=mesh, in_specs=(states, states, *weights), out_specs=(states, *own), check_vma=False)
```

```python
import functools

import jax
import jax.numpy as jnp
from jax import lax
from jax.experimental import pallas as pl
from jax.experimental.pallas import tpu as pltpu
from jax.sharding import PartitionSpec as P

NEG = -1e30
HIDDEN = 2 * NEG
LOG2E = 1.4426950408889634
LIMIT = 67043328
STRIP = 512
HEAD = 256
HALF = HEAD // 2
QUERIES = 2
THETA = 10000
DEVICES = 8
BLOCK = 384
TOKENS = DEVICES * BLOCK
SCALE = HEAD**-0.5
LOW = jnp.bfloat16
WIDE = jnp.float32
NATURAL = tuple(range(DEVICES))
IN_ORDER = ((0, 1), (2, 3, 4, 5), (6, 7))
BY_ARRIVAL = ((0, 1), (2, 4), (3, 5, 6, 7))
ARRIVAL = sum(BY_ARRIVAL, ())


def dot(a, b, ca=1, cb=0):
    return lax.dot_general(a, b, (((ca,), (cb,)), ((), ())), preferred_element_type=WIDE)


def rounded(total, *arrived):
    for t in arrived:
        total = total + t.astype(WIDE)
    return total.astype(LOW)


def params():
    return pltpu.CompilerParams(dimension_semantics=("arbitrary",), vmem_limit_bytes=LIMIT)


def _start(copies):
    for c in copies:
        c.start()


def _wait(copies):
    for c in copies:
        c.wait()


HBM = pl.BlockSpec(memory_space=pltpu.HBM)


def _masks(bq, bk):
    cols = QUERIES * bq
    return lax.rem(lax.broadcasted_iota(jnp.int32, (bk, cols), 1), bq) - lax.broadcasted_iota(jnp.int32, (bk, cols), 0)


def _blocks(iq, bq, bk, block):
    whole, last = lax.div(iq * bq + 1, bk), lax.div(iq * bq + bq + bk - 1, bk)
    lax.fori_loop(0, whole, lambda j, _: block(j, False), None)
    lax.fori_loop(whole, last, lambda j, _: block(j, True), None)


def _row(ref):
    return jnp.concatenate([ref[n : n + 1, :] for n in range(QUERIES)], axis=1)


def _forward(place_ref, q_ref, k_ref, v_ref, o_ref, lse_ref, top_s, mix_s, gap_s, o_s, sem, *, bq, bk):
    cols = QUERIES * bq
    iq = pl.program_id(0)
    slot, last = lax.rem(iq, 2), pl.num_programs(0) - 1
    e = SCALE * LOG2E
    pieces = range(0, cols, STRIP)

    @pl.when(iq == 0)
    def _():
        gap_s[...] = _masks(bq, bk)

    def copies(i, slot):
        per = bq // BLOCK
        return [pltpu.make_async_copy(o_s.at[slot, pl.ds(n * BLOCK, BLOCK), :], o_ref.at[pl.ds(place_ref[i * per + n] * BLOCK, BLOCK), :], sem.at[slot, n])
                for n in range(per)]

    top_s[...] = jnp.full((1, cols), NEG, WIDE)
    mix_s[...] = jnp.zeros_like(mix_s)
    ones = jnp.ones((8, bk), LOW)

    def block(j, masked):
        here = pl.ds(j * bk, bk)
        scores = [dot(k_ref[here, :], q_ref[...].reshape(cols, HEAD)[at : at + STRIP, :], 1, 1) for at in pieces]
        ok = gap_s[...] >= j * bk - iq * bq if masked else None
        weights, keeps = [], []
        for at, s in zip(pieces, scores):
            if masked:
                s = jnp.where(ok[:, at : at + STRIP], s, HIDDEN)
            old = top_s[:, at : at + STRIP]
            top = jnp.maximum(old, s.max(axis=0, keepdims=True))
            top_s[:, at : at + STRIP] = top
            weights.append(jnp.exp2((s - top) * e).astype(LOW))
            keeps.append(jnp.exp2((old - top) * e))
        for at, p, keep in zip(pieces, weights, keeps):
            values = jnp.concatenate([v_ref[here, :].T, ones], axis=0)
            mix_s[:, at : at + STRIP] = mix_s[:, at : at + STRIP] * keep + dot(values, p)

    _blocks(iq, bq, bk, block)
    total = mix_s[HEAD : HEAD + 1, :]
    mixed = (mix_s[:HEAD, :] * (1 / total)).T.astype(LOW)

    @pl.when(iq > 1)
    def _():
        _wait(copies(iq - 2, slot))

    for n in range(QUERIES):
        o_s[slot, :, n * HEAD : (n + 1) * HEAD] = mixed[n * bq : (n + 1) * bq]
    _start(copies(iq, slot))
    lse = top_s[...] * SCALE + jnp.log(total)
    for n in range(QUERIES):
        lse_ref[n : n + 1, :] = lse[:, n * bq : (n + 1) * bq]

    @pl.when(iq == last)
    def _():
        _wait(copies(iq - 1, 1 - slot) + copies(iq, slot))


def _queries(bq):
    return pl.BlockSpec((QUERIES, bq, HEAD), lambda i, *_: (0, i, 0)), pl.BlockSpec((QUERIES, bq), lambda i, *_: (0, i))


def _whole(*shape):
    return pl.BlockSpec(shape, lambda i, *_: (0,) * len(shape))


def _attention_cost(width):
    n = QUERIES * TOKENS * TOKENS
    return pl.CostEstimate(flops=n * width * HEAD, transcendentals=n // 2, bytes_accessed=12 * TOKENS * HEAD)


def attend(place, q, k, v, bq=768, bk=768):
    heads, stats = _queries(bq)
    return pl.pallas_call(
        functools.partial(_forward, bq=bq, bk=bk),
        grid_spec=pltpu.PrefetchScalarGridSpec(
            num_scalar_prefetch=1,
            grid=(TOKENS // bq,),
            in_specs=[heads, _whole(TOKENS, HEAD), _whole(TOKENS, HEAD)],
            out_specs=[HBM, stats],
            scratch_shapes=[pltpu.VMEM((1, QUERIES * bq), WIDE), pltpu.VMEM((HEAD + 8, QUERIES * bq), WIDE),
                            pltpu.VMEM((bk, QUERIES * bq), jnp.int32), pltpu.VMEM((2, bq, QUERIES * HEAD), LOW),
                            pltpu.SemaphoreType.DMA((2, bq // BLOCK))],
        ),
        out_shape=[jax.ShapeDtypeStruct((TOKENS, QUERIES * HEAD), LOW), jax.ShapeDtypeStruct(q.shape[:2], WIDE)],
        compiler_params=params(),
        cost_estimate=_attention_cost(2),
    )(place, q, k, v)


def _backward(place_ref, do_place_ref, q_ref, k_ref, v_ref, *refs, bq, bk):
    per = bq // BLOCK
    o_refs, do_refs = refs[:per], refs[per : 2 * per]
    lse_ref, dq_ref, dk_ref, dv_ref, dq_s, dk_s, dv_s, gap_s, do_s, delta_s = refs[2 * per :]
    cols = QUERIES * bq
    iq = pl.program_id(0)
    e = SCALE * LOG2E
    pieces = range(0, cols, STRIP)

    @pl.when(iq == 0)
    def _():
        gap_s[...] = _masks(bq, bk)
        dk_s[...] = jnp.zeros_like(dk_s)
        dv_s[...] = jnp.zeros_like(dv_s)

    dq_s[...] = jnp.zeros_like(dq_s)
    lses = _row(lse_ref) * LOG2E
    for n in range(QUERIES):
        for i in range(per):
            at, columns = n * bq + i * BLOCK, slice(n * HEAD, (n + 1) * HEAD)
            d_out = do_refs[i][:, columns]
            do_s[at : at + BLOCK, :] = d_out
            both = d_out.astype(WIDE) * o_refs[i][:, columns].astype(WIDE)
            delta_s[:, at : at + BLOCK] = (both[:, :HALF] + both[:, HALF:]).T.sum(axis=0, keepdims=True)
    deltas = delta_s[...]

    def block(j, masked):
        here = pl.ds(j * bk, bk)
        qs = [q_ref[...].reshape(cols, HEAD)[at : at + STRIP, :] for at in pieces]
        dos = [do_s[at : at + STRIP, :] for at in pieces]
        scores = [dot(k_ref[here, :], x, 1, 1) for x in qs]
        dps = [dot(v_ref[here, :], x, 1, 1) for x in dos]
        ok = gap_s[...] >= j * bk - iq * bq if masked else None
        for n, at in enumerate(pieces):
            p = jnp.exp2(scores[n] * e - lses[:, at : at + STRIP])
            if masked:
                p = jnp.where(ok[:, at : at + STRIP], p, 0.0)
            ds = (p * (dps[n] - deltas[:, at : at + STRIP])).astype(LOW)
            dv_s[here, :] += dot(p.astype(LOW), dos[n])
            dk_s[here, :] += dot(ds, qs[n])
            dq_s[:, at : at + STRIP] += dot(k_ref[here, :].T, ds)

    _blocks(iq, bq, bk, block)
    dq_ref[...] = (dq_s[...] * SCALE).T.reshape(QUERIES, bq, HEAD).astype(LOW)

    @pl.when(iq == pl.num_programs(0) - 1)
    def _():
        dk_ref[...] = (dk_s[...] * SCALE).astype(LOW)
        dv_ref[...] = dv_s[...].astype(LOW)


def attend_back(place, do_place, q, k, v, out, d_out, lse, bq=768, bk=768):
    heads, stats = _queries(bq)
    keys = _whole(TOKENS, HEAD)
    per = bq // BLOCK
    outs = [pl.BlockSpec((BLOCK, QUERIES * HEAD), lambda i, place, _, n=n: (place[i * per + n], 0)) for n in range(per)]
    d_outs = [pl.BlockSpec((BLOCK, QUERIES * HEAD), lambda i, _, place, n=n: (place[i * per + n], 0)) for n in range(per)]
    return pl.pallas_call(
        functools.partial(_backward, bq=bq, bk=bk),
        grid_spec=pltpu.PrefetchScalarGridSpec(
            num_scalar_prefetch=2,
            grid=(TOKENS // bq,),
            in_specs=[heads, keys, keys, *outs, *d_outs, stats],
            out_specs=[heads, keys, keys],
            scratch_shapes=[pltpu.VMEM((HEAD, QUERIES * bq), WIDE), pltpu.VMEM((TOKENS, HEAD), WIDE), pltpu.VMEM((TOKENS, HEAD), WIDE),
                            pltpu.VMEM((bk, QUERIES * bq), jnp.int32), pltpu.VMEM((QUERIES * bq, HEAD), LOW), pltpu.VMEM((1, QUERIES * bq), WIDE)],
        ),
        out_shape=[jax.ShapeDtypeStruct(t.shape, LOW) for t in (q, k, v)],
        compiler_params=params(),
        cost_estimate=_attention_cost(5),
    )(place, do_place, q, k, v, *[out] * per, *[d_out] * per, lse)


def _of_groups(refs, groups, store):
    first = 0
    for ref, group in zip(refs, groups):
        last = first + len(group)
        pl.when((pl.program_id(0) >= first) & (pl.program_id(0) < last))(functools.partial(store, ref))
        first = last


def _turn(own_ref, *refs):
    groups, (cos_ref, sin_ref, q_ref, k_ref, v_ref) = refs[:-5], refs[-5:]

    def store(t_ref):
        cos, sin = cos_ref[...], sin_ref[...]
        for n, to in enumerate((q_ref.at[0], q_ref.at[1], k_ref)):
            a = t_ref[:, n * HEAD : n * HEAD + HALF].astype(WIDE)
            b = t_ref[:, n * HEAD + HALF : (n + 1) * HEAD].astype(WIDE)
            to[:, :HALF] = (a * cos - b * sin).astype(LOW)
            to[:, HALF:] = (b * cos + a * sin).astype(LOW)
        v_ref[...] = t_ref[:, 3 * HEAD :]

    _of_groups(groups, IN_ORDER, store)


def _turn_back(own_ref, q_ref, k_ref, v_ref, cos_ref, sin_ref, t_ref):
    cos, sin = cos_ref[...], sin_ref[...]
    for n, of in enumerate((q_ref.at[0], q_ref.at[1], k_ref)):
        a, b = of[:, :HALF].astype(WIDE), of[:, HALF:].astype(WIDE)
        t_ref[:, n * HEAD : n * HEAD + HALF] = (a * cos + b * sin).astype(LOW)
        t_ref[:, n * HEAD + HALF : (n + 1) * HEAD] = (b * cos - a * sin).astype(LOW)
    t_ref[:, 3 * HEAD :] = v_ref[...]


def by_blocks(kernel, given, outs, groups=(NATURAL,)):
    sizes = [len(group) for group in groups]
    spans = iter([(sum(sizes[:n]), size) for n, size in enumerate(sizes)])

    def spec(shape):
        if len(shape) == 3:
            return pl.BlockSpec((shape[0], BLOCK, shape[2]), lambda s, own: (0, own[s], 0))
        if shape[1] <= HEAD:
            return pl.BlockSpec((BLOCK, shape[1]), lambda s, own: (own[s], 0))
        first, size = next(spans)
        return pl.BlockSpec((BLOCK, shape[1]), lambda s, own: (jnp.clip(s - first, 0, size - 1), 0))

    size = sum(2 * a.size for a in given)
    return pl.pallas_call(
        kernel,
        grid_spec=pltpu.PrefetchScalarGridSpec(num_scalar_prefetch=1, grid=(DEVICES,), in_specs=[spec(a.shape) for a in given],
                                               out_specs=[spec(s) for s in outs]),
        out_shape=[jax.ShapeDtypeStruct(s, LOW) for s in outs],
        compiler_params=params(),
        cost_estimate=pl.CostEstimate(flops=4 * size, transcendentals=0, bytes_accessed=2 * size),
    )(owners(sum(groups, ())), *given)


class Turns:
    def __init__(self):
        self.last = []

    def done(self, *results):
        self.last = list(results)


class Sources:
    def __init__(self, turns):
        self.arrays = []
        self.turns = turns

    def add(self, piece):
        t, at, n = piece
        for i, other in enumerate(self.arrays):
            if other is t:
                return i, at, n
        self.arrays.append(t)
        return len(self.arrays) - 1, at, n

    def close(self):
        for t in self.turns.last:
            self.add((t, 0, 0))


def _fetch(refs, pieces, to, sem, columns=slice(None)):
    copies, row = [], 0
    for i, (which, at, n) in enumerate(pieces):
        copies.append(pltpu.make_async_copy(refs[which].at[pl.ds(at, n), columns], to.at[pl.ds(row, n), :], sem.at[i]))
        row += n
    return copies


def _spans(pieces):
    row = 0
    for _, _, n in pieces:
        yield row, n
        row += n


def _tile_of(step, tile):
    return pl.ds(pl.multiple_of(step * tile, tile), tile)


def rows_times(turns, lhs, weights, flip, tile, finish, given, outs, into=None, at=None):
    sources = Sources(turns)
    lhs = [[sources.add(p) for p in pieces] for pieces in lhs]
    sources.close()
    spans = list(_spans(lhs[0]))
    total_rows = sum(n for _, n in spans)
    widths = [w.shape[1] if flip else w.shape[0] for w in weights]
    n_out = weights[0].shape[0] if flip else weights[0].shape[1]
    n_src, n_w, n_l, n_in = len(sources.arrays), len(weights), len(lhs), len(given)
    steps = n_out // tile
    given_too = [] if into is None else [into]

    def kernel(*refs):
        src, ws, ins, rest = refs[:n_src], refs[n_src : n_src + n_w], refs[n_src + n_w : n_src + n_w + n_in], refs[n_src + n_w + n_in + len(given_too) :]
        out_refs, rest = rest[: len(outs)], rest[len(outs) :]
        held, slots, sems, slot_sem = rest[:n_l], rest[n_l : n_l + n_w], rest[n_l + n_w : -1], rest[-1]
        j = pl.program_id(0)
        slot = lax.rem(j, 2)

        def tiles(step, slot):
            here = _tile_of(step, tile)
            return [pltpu.make_async_copy(w.at[here, :] if flip else w.at[:, here], s.at[slot], slot_sem.at[slot, i])
                    for i, (w, s) in enumerate(zip(ws, slots))]

        def multiply(row, n):
            here = pl.ds(row, n)
            terms = [dot(held[min(i, n_l - 1)][here, :], slots[i][slot], 1, 1 if flip else 0) for i in range(n_w)]
            finish(terms, row, n, ins, out_refs)

        @pl.when(j == 0)
        def _():
            copies = [_fetch(src, pieces, to, sem) for pieces, to, sem in zip(lhs, held, sems)]
            first = tiles(0, 0)
            _start([first[0], *(c[0] for c in copies), *first[1:]])
            for i in range(1, len(spans)):
                _start([c[i] for c in copies])
            _wait(first)
            for i, span in enumerate(spans):
                _wait([c[i] for c in copies])
                if i == len(spans) - 1 and steps > 1:
                    _start(tiles(1, 1))
                multiply(*span)

        @pl.when((j > 0) & (j + 1 < steps))
        def _():
            _start(tiles(j + 1, 1 - slot))

        @pl.when(j > 0)
        def _():
            _wait(tiles(j, slot))
            for row in range(0, total_rows, 2 * BLOCK):
                multiply(row, 2 * BLOCK)

    columns = lambda n: pl.BlockSpec((n, tile), lambda j: (0, j))
    wide = sum(widths)
    got = pl.pallas_call(
        kernel,
        grid=(steps,),
        in_specs=[HBM] * (n_src + n_w) + [columns(t.shape[0]) for t in given] + [HBM] * len(given_too),
        input_output_aliases={n_src + n_w + n_in: 0} if given_too else {},
        out_specs=[columns(n) if at is None else pl.BlockSpec((n, tile), lambda j: (at, j)) for n in outs],
        out_shape=[jax.ShapeDtypeStruct((n if at is None else TOKENS, n_out), LOW) for n in outs],
        scratch_shapes=[pltpu.VMEM((total_rows, w), LOW) for w in widths[:n_l]]
        + [pltpu.VMEM((2, tile, w) if flip else (2, w, tile), LOW) for w in widths]
        + [pltpu.SemaphoreType.DMA((len(spans),))] * n_l + [pltpu.SemaphoreType.DMA((2, n_w))],
        compiler_params=params(),
        cost_estimate=pl.CostEstimate(flops=2 * total_rows * wide * n_out, transcendentals=0,
                                      bytes_accessed=2 * (wide * n_out + total_rows * (wide + n_out))),
    )(*sources.arrays, *weights, *given, *given_too)
    turns.done(got[-1])
    return got


def product(turns, lhs, weights, flip, arrived=None, tile=512, joint=False, into=None, at=None):
    sizes = [n for _, _, n in lhs[0]]
    arrived = arrived or [()] * len(sizes)

    def finish(terms, row, n, ins, outs):
        total = sum(terms[1:], terms[0])
        if joint:
            outs[0][pl.ds(row, n), :] = total.astype(LOW)
            return
        ins = iter(ins)
        for (at, size), ts, out in zip(_spans(lhs[0]), arrived, outs):
            mine = [next(ins) for _ in ts]
            if row <= at < row + n:
                out[...] = rounded(total[at - row : at - row + size], *(t[...] for t in mine))

    got = rows_times(turns, lhs, weights, flip, tile, finish, [t for ts in arrived for t in ts], [sum(sizes)] if joint else sizes, into, at)
    return got[0] if joint else got


def gated(turns, pieces, w_gate, w_up, back):
    def finish(terms, row, n, ins, outs):
        gate, up = terms
        here = pl.ds(row, n)
        by = ins[0][here, :].astype(WIDE)
        s = jax.nn.sigmoid(gate)
        silu = gate * s
        outs[0][here, :] = (silu * up).astype(LOW)
        outs[1][here, :] = (by * up * (s + silu * (1 - s))).astype(LOW)
        outs[2][here, :] = (by * silu).astype(LOW)

    return rows_times(turns, [pieces], [w_gate, w_up], False, HEAD, finish, [back], [back.shape[0]] * 3)


def weight_gradient(turns, lhs, rhs, hold_lhs, tile=512, splits=None, first=0, last=None, into=None):
    sources = Sources(turns)
    lhs, rhs = [sources.add(p) for p in lhs], [sources.add(p) for p in rhs]
    sources.close()
    n_src = len(sources.arrays)
    wide_l, wide_r = (sources.arrays[t[0][0]].shape[1] for t in (lhs, rhs))
    kept, tiled = (lhs, rhs) if hold_lhs else (rhs, lhs)
    wide_kept, wide_tiled = (wide_l, wide_r) if hold_lhs else (wide_r, wide_l)
    end = wide_tiled // tile if last is None else last
    splits = splits or (wide_r,)

    def kernel(*refs):
        src = refs[:n_src]
        outs = refs[n_src + (into is not None) :][: len(splits)]
        turned, held, slots, sem, slot_sems = refs[-5:]
        i = pl.program_id(0) + first
        slot = lax.rem(i, 2)

        def tiles(step, slot):
            return _fetch(src, tiled, slots.at[slot], slot_sems.at[slot], _tile_of(step, tile))

        def store(total):
            at = 0
            for ref, n in zip(outs, splits if not hold_lhs else (tile,)):
                ref[...] = total[:, at : at + n].astype(LOW)
                at += n

        @pl.when(i == first)
        def _():
            keep, now = _fetch(src, kept, held, sem), tiles(first, first % 2)
            where = list(_spans(tiled))
            for c, (row, n) in zip(keep, _spans(kept)):
                _start([c] + [t for t, (at, _) in zip(now, where) if row <= at < row + n])
            if first + 1 < end:
                _start(tiles(first + 1, 1 - first % 2))
            total = None
            for c, (row, n) in zip(keep, _spans(kept)):
                _wait([c] + [t for t, (at, _) in zip(now, where) if row <= at < row + n])
                here = pl.ds(row, n)
                if hold_lhs:
                    turned[:, here] = held[here, :].T
                    term = dot(turned[:, here], slots[first % 2, here, :])
                else:
                    term = dot(slots[first % 2, here, :], held[here, :], 0, 0)
                total = term if total is None else total + term
            store(total)

        @pl.when((i > first) & (i + 1 < end))
        def _():
            _start(tiles(i + 1, 1 - slot))

        @pl.when(i > first)
        def _():
            _wait(tiles(i, slot))
            store(dot(turned[...], slots[slot]) if hold_lhs else dot(slots[slot], held[...], 0, 0))

    if hold_lhs:
        out_specs, out_shape = [pl.BlockSpec((wide_l, tile), lambda i: (0, i + first))], [(wide_l, wide_r)]
    else:
        out_specs, out_shape = [pl.BlockSpec((tile, n), lambda i: (i + first, 0)) for n in splits], [(wide_l, n) for n in splits]
    done = tile * (end - first)
    got = pl.pallas_call(
        kernel,
        grid=(end - first,),
        in_specs=[HBM] * (n_src + (into is not None)),
        input_output_aliases={} if into is None else {n_src: 0},
        out_specs=out_specs,
        out_shape=[jax.ShapeDtypeStruct(s, LOW) for s in out_shape],
        scratch_shapes=[pltpu.VMEM((wide_l, TOKENS) if hold_lhs else (8, HALF), LOW), pltpu.VMEM((TOKENS, wide_kept), LOW), pltpu.VMEM((2, TOKENS, tile), LOW),
                        pltpu.SemaphoreType.DMA((len(kept),)), pltpu.SemaphoreType.DMA((2, len(tiled)))],
        compiler_params=params(),
        cost_estimate=pl.CostEstimate(flops=2 * TOKENS * wide_kept * done, transcendentals=0,
                                      bytes_accessed=2 * (TOKENS * wide_kept + (TOKENS + wide_kept) * done)),
    )(*sources.arrays, *([] if into is None else [into]))
    turns.done(got[0])
    return got[0] if len(got) == 1 else got


def wholes(ts):
    return [(t, 0, t.shape[0]) for t in ts]


def places(t, ps, n=1):
    return [(t, p * BLOCK, n * BLOCK) for p in ps]


def _u(i):
    return 2 if i % 2 else 4


TO_CORE = [(i, i ^ 1) for i in range(DEVICES)]
TO_U = [(i, i ^ _u(i)) for i in range(DEVICES)]
TO_V = [(i, i ^ (6 - _u(i))) for i in range(DEVICES)]


def send(t, pairs):
    return lax.ppermute(t, "tp", pairs)


def places_of_blocks():
    me = lax.axis_index("tp")
    away = me ^ jnp.arange(DEVICES, dtype=jnp.int32)
    crossed = (away & 1) | ((away & 2) * 2) | ((away & 4) // 2)
    place = jnp.where(me % 2 == 1, crossed, away).astype(jnp.int32)
    return place, jnp.where((place == 3) | (place == 4), 7 - place, place)


def owners(order):
    me = lax.axis_index("tp")
    v = 2 + 2 * (me % 2)
    away = (0, 1, v, v ^ 1, 6 - v, 7 - v, 6, 7)
    return jnp.stack([me ^ away[p] for p in order]).astype(jnp.int32)


def gather(t, behind=None):
    out = t if behind is None else lax.optimization_barrier((t, behind))[0]
    c, u, v = send(t, TO_CORE), send(out, TO_U), send(out, TO_V)
    far = send(v, TO_U)
    return [t, c, v, send(u, TO_CORE), u, send(v, TO_CORE), far, send(far, TO_CORE)]


def scatter(turns, term, meanwhile, apart):
    far, to_core = term((6, 7), ((), ()))
    far_core = send(to_core, TO_CORE)
    v3, u5 = term((3, 5), ((), ()))
    far = rounded(far.astype(WIDE), far_core)
    turns.done(v3, far)
    far = send(far, TO_U)
    v3, u5 = send(v3, TO_CORE), send(u5, TO_CORE)
    if apart:
        via_u, via_v = term((4, 2), ((v3,), (u5,)))
        via_u = send(via_u, TO_U)
        to_core, mine = meanwhile()
        via_v = rounded(via_v.astype(WIDE), far)
        turns.done(via_v)
        return mine, send(to_core, TO_CORE), via_u, send(via_v, TO_V)
    via_u, to_core = term((4, 1), ((v3,), ()))
    via_u, to_core = send(via_u, TO_U), send(to_core, TO_CORE)
    meanwhile()
    via_v, mine = term((2, 0), ((u5, far), ()))
    via_v = send(via_v, TO_V)
    return mine, to_core, via_u, via_v


def by_rows(kernel, given, n_outs, rows=64):
    spec = pl.BlockSpec((rows, given[0].shape[1]), lambda i: (i, 0))
    size = given[0].size * (len(given) + n_outs)
    return pl.pallas_call(
        kernel,
        grid=(given[0].shape[0] // rows,),
        in_specs=[spec] * len(given),
        out_specs=[spec] * n_outs,
        out_shape=[jax.ShapeDtypeStruct(given[0].shape, LOW)] * n_outs,
        compiler_params=params(),
        cost_estimate=pl.CostEstimate(flops=4 * size, transcendentals=0, bytes_accessed=2 * size),
    )(*given)


def scale_of(wide):
    return lax.rsqrt(jnp.mean(wide**2, -1, keepdims=True) + 1e-6)


def normed(h):
    wide = h.astype(WIDE)
    return (wide * scale_of(wide)).astype(LOW)


def _add_and_norm(x_ref, *refs):
    *terms, h_ref, b_ref = refs
    h = rounded(x_ref[...].astype(WIDE), rounded(*(t[...].astype(WIDE) for t in terms)))
    h_ref[...] = h
    b_ref[...] = normed(h)


def _norm_back(h_ref, before_ref, *refs):
    *terms, out_ref = refs
    by = rounded(*(t[...].astype(WIDE) for t in terms)).astype(WIDE)
    wide = h_ref[...].astype(WIDE)
    scale = scale_of(wide)
    shared = scale * scale * jnp.mean(by * wide, -1, keepdims=True)
    out_ref[...] = rounded(before_ref[...].astype(WIDE), ((by - wide * shared) * scale).astype(LOW))


def angles():
    angle = jnp.arange(TOKENS, dtype=WIDE)[:, None] * THETA ** (-jnp.arange(HALF, dtype=WIDE) / HALF)
    return jnp.cos(angle), jnp.sin(angle)


def layer(x, dy, wq, wk, wv, wo, w_gate, w_up, w_down):
    turns = Turns()
    tables = angles()
    w_qkv = jnp.concatenate([wq, wk, wv], 1)
    turns.done(*tables)
    place, arrival = places_of_blocks()

    def by_group(n, groups, of, weight, flip, tile=512, into=None, at=None):
        return product(turns, [wholes([of[p] for p in groups[n]])], [weight], flip, joint=True, tile=tile, into=into, at=at)

    a = gather(normed(x))
    dys = gather(dy, a[6])
    qkv = [by_group(0, IN_ORDER, a, w_qkv, False)]
    by_hidden = [by_group(0, BY_ARRIVAL, dys, w_down, True, HEAD)]
    qkv += [by_group(n, IN_ORDER, a, w_qkv, False) for n in (1, 2)]
    q, k, v = by_blocks(_turn, (*qkv, *tables), ((QUERIES, TOKENS, HEAD), (TOKENS, HEAD), (TOKENS, HEAD)), IN_ORDER)
    heads, lse = attend(place, q, k, v)
    turns.done(heads)

    def hidden_back(n):
        by_hidden.append(by_group(n, BY_ARRIVAL, dys, w_down, True, HEAD))

    def by_heads_out(ps, arrived):
        return product(turns, [places(heads, ps)], [wo], False, arrived, tile=wo.shape[1])

    def meanwhile():
        hidden_back(1)
        return by_heads_out((1, 0), ((), ()))

    terms = scatter(turns, by_heads_out, meanwhile, True)
    hidden_back(2)
    h, b = by_rows(_add_and_norm, (x, *terms), 2)
    b = gather(b)
    hidden, by_gate, by_up = [], [], []

    def of_groups(ts, ps):
        return [next((t, group.index(p) * BLOCK, BLOCK) for t, group in zip(ts, BY_ARRIVAL) if p in group) for p in ps]

    def arranged(ts):
        return wholes([ts[p] for p in ARRIVAL])

    def by_b(ps, arrived):
        return product(turns, [of_groups(by_gate, ps), of_groups(by_up, ps)], [w_gate, w_up], True, arrived)

    for n, group in enumerate(BY_ARRIVAL):
        for ts, t in zip((hidden, by_gate, by_up), gated(turns, wholes([b[p] for p in group]), w_gate, w_up, by_hidden[n])):
            ts.append(t)
        if n == 0:
            early = by_b((1, 0), ((), ()))

    terms = scatter(turns, by_b, lambda: early, True)
    d_down = weight_gradient(turns, wholes(hidden), arranged(dys), True)
    (dh,) = by_rows(_norm_back, (h, dy, *terms), 1)
    dhs = gather(dh)
    by_heads = by_group(0, BY_ARRIVAL, dhs, wo, True, at=0)
    d_gate = weight_gradient(turns, arranged(b), wholes(by_gate), False)
    d_up = weight_gradient(turns, arranged(b), wholes(by_up), False, last=4)
    by_heads = by_group(1, BY_ARRIVAL, dhs, wo, True, into=by_heads, at=1)
    by_heads = by_group(2, BY_ARRIVAL, dhs, wo, True, into=by_heads, at=1)
    dq, dk, dv = attend_back(place, arrival, q, k, v, heads, by_heads, lse)
    (by_qkv,) = by_blocks(_turn_back, (dq, dk, dv, *tables), ((TOKENS, 4 * HEAD),))
    turns.done(by_qkv)
    pairs = range(0, DEVICES, 2)
    d_qkv = []

    def qkv_gradient():
        d_qkv.extend(weight_gradient(turns, wholes(a), places(by_qkv, pairs, 2), False, splits=(2 * HEAD, HEAD, HEAD)))

    terms = scatter(turns, lambda ps, arrived: product(turns, [places(by_qkv, ps)], [w_qkv], True, arrived, tile=1792), qkv_gradient, False)
    d_o = weight_gradient(turns, places(heads, pairs, 2), wholes(dhs), True)
    d_up = weight_gradient(turns, arranged(b), wholes(by_up), False, first=4, into=d_up)
    (dx,) = by_rows(_norm_back, (x, dh, *terms), 1)
    return dx, *d_qkv, d_o, d_gate, d_up, d_down


def solution(mesh):
    def step(x, dy, *weights):
        dx, *by_weights = layer(x[0], dy[0], *weights)
        return dx[None], *by_weights

    states, by_columns, by_rows = P("dp", "tp", None), P(None, "tp"), P("tp", None)
    weights = (by_columns, by_columns, by_columns, by_rows, by_columns, by_columns, by_rows)
    own = tuple(P("dp", "tp") if spec == by_columns else P(("dp", "tp"), None) for spec in weights)
    return jax.shard_map(step, mesh=mesh, in_specs=(states, states, *weights), out_specs=(states, *own), check_vma=False)
```
